32 devices in a mesh: date: 16 (over z, y, x), prod: 2 (over core).
Axes of the slice: x: 2, y: 2, z: 4, core: 2. Of those that a mesh axis runs over, the one named last changes fastest.
Arguments:
- daily_sales: float32 [256, 512, 128], P('prod', 'date'), may hold values from -2.5 to 2.5
- week_id: int32 [512], P('date'), may hold values from 0 to 102, never falling along the last dimension, each value on 1 to 7 neighbouring positions
- month_id: int32 [512], P('date'), may hold values from 0 to 21, never falling along the last dimension, each value on 1 to 31 neighbouring positions
- year_id: int32 [512], P('date'), may hold values from 0 to 1, never falling along the last dimension, each value on 1 to 366 neighbouring positions
Outputs:
- running: float32 [256, 512, 128], P('prod', 'date')
- week_total: float32 [256, 512, 128], P('prod', 'date')
- month_total: float32 [256, 512, 128], P('prod', 'date')
- year_total: float32 [256, 512, 128], P('prod', 'date')
- store_rollup: float32 [4, 512, 128], P(None, 'date')
The draws below stay inside these ranges and needn't reach their ends.
Inputs may be any that keep to these rules, and one draw needn't show every extreme that they name: `week_id`: starts at 0 and never falls along the dates; each week covers 1 to 7 consecutive dates and some cover exactly 7. `month_id`: starts at 0 and never falls along the dates; each month covers 1 to 31 consecutive dates and some cover exactly 31; months need not line up with weeks. `year_id`: starts at 0 and never falls along the dates; each year covers 1 to 366 consecutive dates and some cover exactly 366; years need not line up with weeks or months.
All inputs are finite; a program needn't handle non-finite values.
Results may differ from the reference program's by a relative error of at most 0.000094.
Values sent between devices are 32-bit elements.
A program may use at most 64 MiB of HBM per device.

```python
import math
import jax
import jax.numpy as jnp
import numpy as np

PRODUCTS = 256
STORES = 128
DATES = 512


def shard_levels(stream_key, extent, split, low, high):
    loudness = 1.0
    for position, shards_of in split:
        steps = jax.random.uniform(jax.random.fold_in(jax.random.fold_in(stream_key, 6), position), (shards_of,), jnp.float32, low / len(split), high / len(split))
        loudness = loudness * jnp.repeat(jnp.exp(steps), extent[position] // shards_of).reshape((-1,) + (1,) * (len(extent) - 1 - position))
    return loudness


def split_up(number_of, total, reach, lean):
    portions = [(1 << 20) // math.isqrt(rank ** lean) + 1 for rank in range(2, number_of + 1)]
    rest, holding = total - reach - (number_of - 1), [1] * (number_of - 1)
    while rest > 0:
        movable = [i for i in range(number_of - 1) if holding[i] < reach]
        mass, remaining = sum([portions[i] for i in movable]), rest
        for i in movable:
            extra = min(reach - holding[i], max(1, remaining * portions[i] // mass), rest)
            holding[i] = holding[i] + extra
            rest = rest - extra
    return np.array([reach] + holding)


def uneven_parts(stream_key, amount, total, limit, slope):
    if amount == 2:
        one = jax.random.randint(stream_key, (), max(1, total - limit), min(limit, total - 1) + 1)
        return jnp.stack([one, total - one])
    tallies = jnp.asarray(split_up(amount, total, limit, slope), jnp.int32)
    pairs = (amount - 1) // 2
    giver, sink = tallies[1:1 + 2 * pairs:2], tallies[2:2 + 2 * pairs:2]
    room = jnp.minimum(giver - 1, limit - sink)
    passed = jax.random.randint(jax.random.fold_in(stream_key, 1), (pairs,), 0, 1 << 20) % (room + 1)
    tallies = tallies.at[1:1 + 2 * pairs:2].set(giver - passed).at[2:2 + 2 * pairs:2].set(sink + passed)
    return tallies[jax.random.permutation(jax.random.fold_in(stream_key, 2), amount)]


def normal_values(own_key, shape, deviation, limit, pieces=(), kind=jnp.bfloat16):
    factor_of = shard_levels(own_key, shape, pieces, -0.22, 0.18) if pieces else 1.0
    result = jax.random.normal(own_key, shape, jnp.float32) * deviation * factor_of
    return jnp.minimum(jnp.maximum(result, -limit), limit).astype(kind)


def setup_inputs(seed: int = 0) -> dict:
    seeds = jax.random.split(jax.random.key(seed), 5)
    return {
        "daily_sales": normal_values(seeds[0], (PRODUCTS, DATES, STORES), 0.25, 2.5, ((0, 2), (1, 16)), jnp.float32),
        "week_id": jnp.searchsorted(jnp.cumsum(uneven_parts(seeds[1], DATES // 5 + 1, DATES, 7, 0)), jnp.arange(DATES), side="right").astype(jnp.int32),
        "month_id": jnp.searchsorted(jnp.cumsum(uneven_parts(seeds[2], DATES // 24 + 1, DATES, 31, 0)), jnp.arange(DATES), side="right").astype(jnp.int32),
        "year_id": jnp.searchsorted(jnp.cumsum(uneven_parts(seeds[3], DATES // 300 + 1, DATES, 366, 0)), jnp.arange(DATES), side="right").astype(jnp.int32),
    }


def segment_totals(daily_sales, level_ids):
    by_date = jnp.moveaxis(daily_sales, 1, 0)
    seg_sums = jax.ops.segment_sum(by_date, level_ids, num_segments=DATES)
    return jnp.moveaxis(seg_sums[level_ids], 0, 1)


def reference(daily_sales, week_id, month_id, year_id):
    running = jnp.cumsum(daily_sales, axis=1)
    week_total = segment_totals(daily_sales, week_id)
    month_total = segment_totals(daily_sales, month_id)
    year_total = segment_totals(daily_sales, year_id)
    store_rollup = jnp.stack([jnp.sum(running, axis=0), jnp.sum(week_total, axis=0), jnp.sum(month_total, axis=0), jnp.sum(year_total, axis=0)])
    return running, week_total, month_total, year_total, store_rollup
```

```python
import functools

import jax
import jax.numpy as jnp
from jax import lax
from jax.experimental import pallas as pl
from jax.experimental.pallas import tpu as pltpu
from jax.sharding import PartitionSpec as P

MESH = pl.DeviceIdType.MESH
F32 = jnp.float32


def id_column(ids, span, lanes):
    where = lax.broadcasted_iota(jnp.int32, (span, lanes), 0)
    column = jnp.zeros((span, lanes), jnp.int32)
    for t in range(span):
        column = jnp.where(where == t, ids[t], column)
    return column


def id_row(ids, span, lanes):
    where = lax.broadcasted_iota(jnp.int32, (span, lanes), 1) % span
    row = jnp.zeros((span, lanes), jnp.int32)
    for t in range(span):
        row = jnp.where(where == t, ids[t], row)
    return row


def edge_masks(ids, span, lanes):
    column = id_column(ids, span, lanes)
    return (column == ids[0]).astype(F32), (column == ids[span - 1]).astype(F32)


def stack_rows(values, rows, lanes):
    where = lax.broadcasted_iota(jnp.int32, (rows, lanes), 0)
    tile = jnp.zeros((rows, lanes), F32)
    for i, value in enumerate(values):
        tile = jnp.where(where == i, value, tile)
    return tile


def exchange_kernel(
    n, n_prod, slices, loads,
    week, month, year, x_hbm,
    carry, near, meta,
    x, send1, recv1, send2, edges, sib,
    load_sem, s1_sem, r1_sem, s2_sem, r2_sem, sib_s, sib_r, near_s, near_r,
):
    me = lax.axis_index("date")
    core = lax.axis_index("prod")
    columns, span, lanes = x.shape
    rows = columns // slices
    chunk = columns // loads
    loaded = [
        pltpu.make_async_copy(
            x_hbm.at[pl.ds(i * chunk, chunk)], x.at[pl.ds(i * chunk, chunk)], load_sem.at[i]
        )
        for i in range(loads)
    ]
    for copy in loaded:
        copy.start()
    barrier = pltpu.get_barrier_semaphore()
    for d in range(1, n):
        pl.semaphore_signal(
            barrier, inc=1, device_id=(lax.rem(me + d, n), core), device_id_type=MESH
        )
    for d in range(1, n_prod):
        pl.semaphore_signal(
            barrier, inc=1, device_id=(me, lax.rem(core + d, n_prod)), device_id_type=MESH
        )
    head_y, tail_y = edge_masks(year, span, lanes)
    last = span - 1
    ids = stack_rows(
        [
            v.astype(F32)
            for v in (year[0], year[last], week[0], week[last], month[0], month[last])
        ],
        rows, lanes,
    )

    def outer_sums(s, total):
        block = x[pl.ds(pl.multiple_of(s * rows, rows), rows)]
        send1[s, 0] = jnp.sum(block, axis=1)
        send1[s, 1] = jnp.sum(block * head_y[None], axis=1)
        send1[s, 2] = jnp.sum(block * tail_y[None], axis=1)
        send1[s, 3] = ids
        return total + jnp.sum(block, axis=0)

    total = jnp.zeros((span, lanes), F32)
    per_load = slices // loads
    for i in range(loads):
        loaded[i].wait()
        total = lax.fori_loop(i * per_load, (i + 1) * per_load, outer_sums, total)
    sib[core] = total
    pl.semaphore_wait(barrier, n - 1 + n_prod - 1)

    first = []
    for d in range(1, n):
        peer = lax.rem(me + d, n)
        copy = pltpu.make_async_remote_copy(
            src_ref=send1.at[lax.rem(peer, slices)], dst_ref=recv1.at[me],
            send_sem=s1_sem.at[peer], recv_sem=r1_sem.at[me],
            device_id=(peer, core), device_id_type=MESH,
        )
        copy.start()
        first.append(copy)
    shared = []
    for d in range(1, n_prod):
        peer = lax.rem(core + d, n_prod)
        copy = pltpu.make_async_remote_copy(
            src_ref=sib.at[core], dst_ref=sib.at[core],
            send_sem=sib_s.at[peer], recv_sem=sib_r.at[core],
            device_id=(me, peer), device_id_type=MESH,
        )
        copy.start()
        shared.append(copy)

    head_w, tail_w = edge_masks(week, span, lanes)
    head_m, tail_m = edge_masks(month, span, lanes)

    def inner_sums(s, nothing):
        at = pl.ds(pl.multiple_of(s * rows, rows), rows)
        block = x[at]
        edges[0, 0, at] = jnp.sum(block * tail_w[None], axis=1)
        edges[0, 1, at] = jnp.sum(block * tail_m[None], axis=1)
        edges[1, 0, at] = jnp.sum(block * head_w[None], axis=1)
        edges[1, 1, at] = jnp.sum(block * head_m[None], axis=1)
        return nothing

    lax.fori_loop(0, slices, inner_sums, 0)
    left, right = lax.rem(me + n - 1, n), lax.rem(me + 1, n)
    beside = []
    for side, peer in ((0, right), (1, left)):
        copy = pltpu.make_async_remote_copy(
            src_ref=edges.at[side], dst_ref=near.at[side],
            send_sem=near_s.at[side], recv_sem=near_r.at[side],
            device_id=(peer, core), device_id_type=MESH,
        )
        copy.start()
        beside.append(copy)

    recv1[me] = send1[lax.rem(me, slices)]
    for d in range(1, n_prod):
        peer = lax.rem(core + d, n_prod)
        pltpu.make_async_remote_copy(
            src_ref=sib.at[core], dst_ref=sib.at[peer],
            send_sem=sib_s.at[peer], recv_sem=sib_r.at[peer],
            device_id=(me, peer), device_id_type=MESH,
        ).wait_recv()
    whole = sib[0]
    for i in range(1, n_prod):
        whole = whole + sib[i]
    sums = stack_rows(
        [
            jnp.sum(whole * m, axis=0, keepdims=True)
            for m in (jnp.ones_like(head_y), head_y, tail_y, head_w, tail_w, head_m, tail_m)
        ],
        rows, lanes,
    )

    def arrived(buffer, send_sem, recv_sem):
        for d in range(1, n):
            peer = lax.rem(me + d, n)
            pltpu.make_async_remote_copy(
                src_ref=send1.at[0], dst_ref=buffer.at[peer],
                send_sem=send_sem.at[peer], recv_sem=recv_sem.at[peer],
                device_id=(peer, core), device_id_type=MESH,
            ).wait_recv()

    arrived(recv1, s1_sem, r1_sem)
    low = [recv1[b, 3, 0:1, :] for b in range(n)]
    top = [recv1[b, 3, 1:2, :] for b in range(n)]
    running = jnp.zeros((rows, lanes), F32)
    into = jnp.zeros((rows, lanes), F32)
    for b in range(n):
        send2[b, 0] = running
        send2[b, 1] = into
        send2[b, 3] = sums
        if b + 1 < n:
            running = running + recv1[b, 0]
            held = recv1[b, 2] + jnp.where(low[b] == top[b], into, 0.0)
            into = jnp.where(top[b] == low[b + 1], held, 0.0)
    back = jnp.zeros((rows, lanes), F32)
    for b in reversed(range(n)):
        send2[b, 2] = back
        if b > 0:
            held = recv1[b, 1] + jnp.where(low[b] == top[b], back, 0.0)
            back = jnp.where(top[b - 1] == low[b], held, 0.0)

    second = []
    for d in range(1, n):
        peer = lax.rem(me + d, n)
        copy = pltpu.make_async_remote_copy(
            src_ref=send2.at[peer], dst_ref=carry.at[me],
            send_sem=s2_sem.at[peer], recv_sem=r2_sem.at[me],
            device_id=(peer, core), device_id_type=MESH,
        )
        copy.start()
        second.append(copy)
    carry[me] = send2[me]
    arrived(carry, s2_sem, r2_sem)

    zero = jnp.zeros((1, lanes), F32)
    run_sum, in_sum, back_sum = zero, zero, zero
    low_me, top_me = year[0].astype(F32), year[last].astype(F32)
    for b in range(n):
        tile = carry[b, 3]
        run_sum = run_sum + jnp.where(b < me, tile[0:1], 0.0)
        inside = jnp.logical_and(top[b] == low_me, b < me)
        in_sum = in_sum + jnp.where(inside, tile[2:3], 0.0)
        inside = jnp.logical_and(low[b] == top_me, b > me)
        back_sum = back_sum + jnp.where(inside, tile[1:2], 0.0)
    left_ids, right_ids = recv1[left, 3], recv1[right, 3]
    left_sums, right_sums = carry[left, 3], carry[right, 3]

    def gain(seen, own, there):
        return jnp.where(jnp.logical_and(seen == own.astype(F32), there), 1.0, 0.0)

    week_l = gain(left_ids[3:4], week[0], me > 0)
    month_l = gain(left_ids[5:6], month[0], me > 0)
    week_r = gain(right_ids[2:3], week[last], me < n - 1)
    month_r = gain(right_ids[4:5], month[last], me < n - 1)
    meta[0:8] = stack_rows(
        [
            run_sum, in_sum, back_sum,
            left_sums[4:5] * week_l, left_sums[6:7] * month_l,
            right_sums[3:4] * week_r, right_sums[5:6] * month_r,
        ],
        8, lanes,
    )
    meta[8:16] = stack_rows([week_l, month_l, week_r, month_r], 8, lanes)
    meta[16 : 16 + span] = whole
    for copy in beside:
        copy.wait()
    for copy in first + shared + second:
        copy.wait_send()


def exchange(n, n_prod, slices, week, month, year, sales):
    columns, span, lanes = sales.shape
    rows = columns // slices
    loads = 4 if slices % 4 == 0 else 1
    smem = pl.BlockSpec(memory_space=pltpu.SMEM)
    vmem = pl.BlockSpec(memory_space=pltpu.VMEM)
    anywhere = pl.BlockSpec(memory_space=pl.ANY)
    packet = (n, 4, rows, lanes)
    dma = pltpu.SemaphoreType.DMA
    return pl.pallas_call(
        functools.partial(exchange_kernel, n, n_prod, slices, loads),
        out_shape=(
            jax.ShapeDtypeStruct(packet, F32),
            jax.ShapeDtypeStruct((2, 2, columns, lanes), F32),
            jax.ShapeDtypeStruct((16 + span, lanes), F32),
        ),
        in_specs=[smem, smem, smem, anywhere],
        out_specs=(vmem, anywhere, vmem),
        scratch_shapes=[
            pltpu.VMEM(sales.shape, F32),
            pltpu.VMEM((slices, 4, rows, lanes), F32),
            pltpu.VMEM(packet, F32),
            pltpu.VMEM(packet, F32),
            pltpu.VMEM((2, 2, columns, lanes), F32),
            pltpu.VMEM((n_prod, span, lanes), F32),
            dma((loads,)), dma((n,)), dma((n,)), dma((n,)), dma((n,)),
            dma((n_prod,)), dma((n_prod,)), dma((2,)), dma((2,)),
        ],
        compiler_params=pltpu.CompilerParams(collective_id=0, has_side_effects=True),
        name="exchange",
    )(week, month, year, sales)


def split3(value):
    high = value.astype(jnp.bfloat16)
    rest = value - high.astype(F32)
    middle = rest.astype(jnp.bfloat16)
    low = (rest - middle.astype(F32)).astype(jnp.bfloat16)
    return jnp.concatenate([high, middle, low], axis=-2)


def apply_kernel(
    week, month, year, x, carry, near, meta,
    run_out, week_out, month_out, year_out, rollup,
    mixer, gains,
):
    _, span, lanes = x.shape
    groups, _, rows, _ = carry.shape

    @pl.when(pl.program_id(0) == 0)
    def _():
        sub = lax.broadcasted_iota(jnp.int32, (span, 3 * span), 0)
        lane = lax.broadcasted_iota(jnp.int32, (span, 3 * span), 1) % span
        mixer[0:span] = jnp.where(lane <= sub, 1.0, 0.0).astype(mixer.dtype)
        for k, ids in enumerate((week, month, year)):
            same = id_column(ids, span, 3 * span) == id_row(ids, span, 3 * span)
            mixer[(k + 1) * span : (k + 2) * span] = jnp.where(same, 1.0, 0.0).astype(mixer.dtype)
            head, tail = edge_masks(ids, span, lanes)
            if k == 0:
                sum_head, sum_tail = head, tail
            gains[2 * k] = head
            gains[2 * k + 1] = tail
        mixed = jnp.dot(mixer[...], split3(meta[16 : 16 + span]), preferred_element_type=F32)
        rollup[0] = mixed[0:span] + meta[0:1]
        rollup[1] = mixed[span : 2 * span] + meta[3:4] * gains[0] + meta[5:6] * gains[1]
        rollup[2] = mixed[2 * span : 3 * span] + meta[4:5] * gains[2] + meta[6:7] * gains[3]
        rollup[3] = mixed[3 * span : 4 * span] + meta[1:2] * gains[4] + meta[2:3] * gains[5]
        gains[0] = gains[0] * meta[8:9]
        gains[1] = gains[1] * meta[10:11]
        gains[2] = gains[2] * meta[9:10]
        gains[3] = gains[3] * meta[11:12]

    def group(g, nothing):
        base = pl.multiple_of(g * rows, rows)
        at = pl.ds(base, rows)
        left_w, left_m = near[0, 0, at], near[0, 1, at]
        right_w, right_m = near[1, 0, at], near[1, 1, at]
        start, year_l, year_r = carry[g, 0], carry[g, 1], carry[g, 2]
        for r in range(0, rows, 2):
            parts = split3(x[pl.ds(base + r, 2)])
            both = jnp.concatenate([parts[0], parts[1]], axis=1)
            mixed = jnp.dot(mixer[...], both, preferred_element_type=F32)
            for j in range(2):
                q = r + j
                row = slice(q, q + 1)
                own = mixed[:, j * lanes : (j + 1) * lanes]
                run_out[base + q] = own[0:span] + start[row]
                week_out[base + q] = (
                    own[span : 2 * span] + left_w[row] * gains[0] + right_w[row] * gains[1]
                )
                month_out[base + q] = (
                    own[2 * span : 3 * span] + left_m[row] * gains[2] + right_m[row] * gains[3]
                )
                year_out[base + q] = (
                    own[3 * span : 4 * span] + year_l[row] * gains[4] + year_r[row] * gains[5]
                )
        return nothing

    lax.fori_loop(0, groups, group, 0)


def apply(slices, week, month, year, sales, carry, near, meta):
    columns, span, lanes = sales.shape
    rows = columns // slices
    steps = 8 if slices % 8 == 0 else 1
    block = columns // steps
    smem = pl.BlockSpec(memory_space=pltpu.SMEM)
    cube = pl.BlockSpec((block, span, lanes), lambda i: (i, 0, 0))
    cube_shape = jax.ShapeDtypeStruct(sales.shape, F32)
    return pl.pallas_call(
        apply_kernel,
        grid=(steps,),
        out_shape=(cube_shape,) * 4 + (jax.ShapeDtypeStruct((4, span, lanes), F32),),
        in_specs=[
            smem, smem, smem, cube,
            pl.BlockSpec((slices // steps, 4, rows, lanes), lambda i: (i, 0, 0, 0)),
            pl.BlockSpec((2, 2, block, lanes), lambda i: (0, 0, i, 0)),
            pl.BlockSpec(meta.shape, lambda i: (0, 0)),
        ],
        out_specs=(cube,) * 4 + (pl.BlockSpec((4, span, lanes), lambda i: (0, 0, 0)),),
        scratch_shapes=[
            pltpu.VMEM((4 * span, 3 * span), jnp.bfloat16),
            pltpu.VMEM((6, span, lanes), F32),
        ],
        compiler_params=pltpu.CompilerParams(dimension_semantics=("arbitrary",)),
        name="apply",
    )(week, month, year, sales, carry, near, meta)


def solution(mesh):
    n, n_prod = mesh.shape["date"], mesh.shape["prod"]

    def local(sales, week, month, year):
        slices = min(n, sales.shape[0] // 8)
        carry, near, meta = exchange(n, n_prod, slices, week, month, year, sales)
        return apply(slices, week, month, year, sales, carry, near, meta)

    return jax.shard_map(
        local,
        mesh=mesh,
        in_specs=(P("prod", "date", None), P("date"), P("date"), P("date")),
        out_specs=(P("prod", "date", None),) * 4 + (P(None, "date", None),),
        check_vma=False,
    )
```

```python
import functools

import jax
import jax.numpy as jnp
from jax import lax
from jax.experimental import pallas as pl
from jax.experimental.pallas import tpu as pltpu
from jax.sharding import PartitionSpec as P

MESH = pl.DeviceIdType.MESH
F32 = jnp.float32


def id_column(ids, span, lanes):
    where = lax.broadcasted_iota(jnp.int32, (span, lanes), 0)
    column = jnp.zeros((span, lanes), jnp.int32)
    for t in range(span):
        column = jnp.where(where == t, ids[t], column)
    return column


def id_row(ids, span, lanes):
    where = lax.broadcasted_iota(jnp.int32, (span, lanes), 1) % span
    row = jnp.zeros((span, lanes), jnp.int32)
    for t in range(span):
        row = jnp.where(where == t, ids[t], row)
    return row


def edge_masks(ids, span, lanes):
    column = id_column(ids, span, lanes)
    return (column == ids[0]).astype(F32), (column == ids[span - 1]).astype(F32)


def stack_rows(values, rows, lanes):
    where = lax.broadcasted_iota(jnp.int32, (rows, lanes), 0)
    tile = jnp.zeros((rows, lanes), F32)
    for i, value in enumerate(values):
        tile = jnp.where(where == i, value, tile)
    return tile


def exchange_kernel(
    n, n_prod, slices, loads, wide,
    week, month, year, x_hbm,
    carry, near, meta, mixer, gains,
    x, send1, recv1, send2, edges, seen, parts,
    load_sem, id_s, id_r, s1_sem, r1_sem, s2_sem, r2_sem, sib_s, sib_r, near_s, near_r,
):
    me = lax.axis_index("date")
    core = lax.axis_index("prod")
    columns, span, lanes = x.shape
    rows = columns // slices
    chunk = columns // loads
    last = span - 1
    loaded = [
        pltpu.make_async_copy(
            x_hbm.at[pl.ds(i * chunk, chunk)], x.at[pl.ds(i * chunk, chunk)], load_sem.at[i]
        )
        for i in range(loads)
    ]
    for copy in loaded:
        copy.start()
    barrier = pltpu.get_barrier_semaphore()
    for d in range(1, n):
        pl.semaphore_signal(
            barrier, inc=1, device_id=(lax.rem(me + d, n), core), device_id_type=MESH
        )
    for d in range(1, n_prod):
        pl.semaphore_signal(
            barrier, inc=1, device_id=(me, lax.rem(core + d, n_prod)), device_id_type=MESH
        )
    lane = lax.broadcasted_iota(jnp.int32, (1, lanes), 1)
    ids = jnp.zeros((1, lanes), F32)
    for i, v in enumerate((year[0], year[last], week[0], week[last], month[0], month[last])):
        ids = jnp.where(lane == i, v.astype(F32), ids)
    seen[me] = ids
    head_y, tail_y = edge_masks(year, span, lanes)

    def outer_sums(s, total):
        block = x[pl.ds(pl.multiple_of(s * rows, rows), rows)]
        send1[s, 0] = jnp.sum(block * head_y[None], axis=1)
        send1[s, 1] = jnp.sum(block * tail_y[None], axis=1)
        if wide:
            send1[s, 2] = jnp.sum(block, axis=1)
        return total + jnp.sum(block, axis=0)

    total = jnp.zeros((span, lanes), F32)
    per_load = slices // loads
    for i in range(loads):
        loaded[i].wait()
        total = lax.fori_loop(i * per_load, (i + 1) * per_load, outer_sums, total)
    recv1[me] = send1[lax.rem(me, slices)]
    pl.semaphore_wait(barrier, n - 1 + n_prod - 1)

    def to_all(source, target, send_sem, recv_sem):
        copies = []
        for d in range(1, n):
            peer = lax.rem(me + d, n)
            copy = pltpu.make_async_remote_copy(
                src_ref=source(peer), dst_ref=target.at[me],
                send_sem=send_sem.at[peer], recv_sem=recv_sem.at[me],
                device_id=(peer, core), device_id_type=MESH,
            )
            copy.start()
            copies.append(copy)
        return copies

    def arrived(target, send_sem, recv_sem):
        for d in range(1, n):
            peer = lax.rem(me + d, n)
            pltpu.make_async_remote_copy(
                src_ref=target.at[me], dst_ref=target.at[peer],
                send_sem=send_sem.at[peer], recv_sem=recv_sem.at[peer],
                device_id=(peer, core), device_id_type=MESH,
            ).wait_recv()

    sent = to_all(lambda peer: seen.at[me], seen, id_s, id_r)
    sent += to_all(lambda peer: send1.at[lax.rem(peer, slices)], recv1, s1_sem, r1_sem)

    left, right = lax.rem(me + n - 1, n), lax.rem(me + 1, n)

    def edge_sums(level, head, tail):
        def inner_sums(s, nothing):
            at = pl.ds(pl.multiple_of(s * rows, rows), rows)
            block = x[at]
            edges[0, level, at] = jnp.sum(block * tail[None], axis=1)
            edges[1, level, at] = jnp.sum(block * head[None], axis=1)
            return nothing

        lax.fori_loop(0, slices, inner_sums, 0)

    def edge_sends(level):
        copies = []
        for side, peer in ((0, right), (1, left)):
            copy = pltpu.make_async_remote_copy(
                src_ref=edges.at[side, level], dst_ref=near.at[side, level],
                send_sem=near_s.at[side, level], recv_sem=near_r.at[side, level],
                device_id=(peer, core), device_id_type=MESH,
            )
            copy.start()
            copies.append(copy)
        return copies

    head_w, tail_w = edge_masks(week, span, lanes)
    edge_sums(0, head_w, tail_w)
    beside = edge_sends(0)
    head_m, tail_m = edge_masks(month, span, lanes)
    edge_sums(1, head_m, tail_m)

    sub = lax.broadcasted_iota(jnp.int32, (span, 3 * span), 0)
    place = lax.broadcasted_iota(jnp.int32, (span, 3 * span), 1) % span
    mixer[0:span] = jnp.where(place <= sub, 1.0, 0.0).astype(mixer.dtype)
    for k, level in enumerate((week, month, year)):
        same = id_column(level, span, 3 * span) == id_row(level, span, 3 * span)
        mixer[(k + 1) * span : (k + 2) * span] = jnp.where(same, 1.0, 0.0).astype(mixer.dtype)

    arrived(seen, id_s, id_r)
    low = [jnp.broadcast_to(seen[b][:, 0:1], (rows, lanes)) for b in range(n)]
    top = [jnp.broadcast_to(seen[b][:, 1:2], (rows, lanes)) for b in range(n)]
    arrived(recv1, s1_sem, r1_sem)
    zero = jnp.zeros((rows, lanes), F32)
    running, into = zero, zero
    brought = []
    for b in range(n):
        send2[b, 0] = running
        brought.append(into)
        if wide:
            send2[b, 1] = into
        if b + 1 < n:
            head, tail = recv1[b, 0], recv1[b, 1]
            one = low[b] == top[b]
            running = running + (recv1[b, 2] if wide else head + jnp.where(one, 0.0, tail))
            into = jnp.where(top[b] == low[b + 1], tail + jnp.where(one, into, 0.0), 0.0)
    back = zero
    for b in reversed(range(n)):
        one = low[b] == top[b]
        if wide:
            send2[b, 2] = back
        else:
            send2[b, 1] = back + jnp.where(one, brought[b], 0.0)
        if b > 0:
            held = recv1[b, 0] + jnp.where(one, back, 0.0)
            back = jnp.where(top[b - 1] == low[b], held, 0.0)
    sent += to_all(lambda peer: send2.at[peer], carry, s2_sem, r2_sem)
    beside += edge_sends(1)
    carry[me] = send2[me]

    def gain(there, lane_seen, own, where):
        value = jnp.broadcast_to(seen[there][:, lane_seen : lane_seen + 1], (1, lanes))
        return jnp.where(jnp.logical_and(value == own.astype(F32), where), 1.0, 0.0)

    gains[0] = head_w * gain(left, 3, week[0], me > 0)
    gains[1] = tail_w * gain(right, 2, week[last], me < n - 1)
    gains[2] = head_m * gain(left, 5, month[0], me > 0)
    gains[3] = tail_m * gain(right, 4, month[last], me < n - 1)
    gains[4] = head_y if wide else head_y * jnp.where(year[0] == year[last], 0.0, 1.0)
    gains[5] = tail_y
    for copy in beside:
        copy.wait_recv()
    arrived(carry, s2_sem, r2_sem)
    kept = carry[0:slices]

    def over_products(value):
        return jnp.sum(value.reshape(columns, lanes), axis=0, keepdims=True)

    parts[core, 0:8] = stack_rows(
        [
            over_products(kept[:, 0]),
            over_products(kept[:, 1 if wide else 0]),
            over_products(kept[:, 2 if wide else 1]),
            over_products(near[0, 0]), over_products(near[0, 1]),
            over_products(near[1, 0]), over_products(near[1, 1]),
        ],
        8, lanes,
    )
    parts[core, 8 : 8 + span] = total
    shared = []
    for d in range(1, n_prod):
        peer = lax.rem(core + d, n_prod)
        copy = pltpu.make_async_remote_copy(
            src_ref=parts.at[core], dst_ref=parts.at[core],
            send_sem=sib_s.at[peer], recv_sem=sib_r.at[core],
            device_id=(me, peer), device_id_type=MESH,
        )
        copy.start()
        shared.append(copy)
    for copy in sent + beside:
        copy.wait_send()
    for d in range(1, n_prod):
        peer = lax.rem(core + d, n_prod)
        pltpu.make_async_remote_copy(
            src_ref=parts.at[core], dst_ref=parts.at[peer],
            send_sem=sib_s.at[peer], recv_sem=sib_r.at[peer],
            device_id=(me, peer), device_id_type=MESH,
        ).wait_recv()
    whole = parts[0]
    for i in range(1, n_prod):
        whole = whole + parts[i]
    meta[...] = whole
    for copy in shared:
        copy.wait_send()


def exchange(n, n_prod, slices, wide, week, month, year, sales):
    columns, span, lanes = sales.shape
    rows = columns // slices
    loads = 4 if slices % 4 == 0 else 1
    smem = pl.BlockSpec(memory_space=pltpu.SMEM)
    vmem = pl.BlockSpec(memory_space=pltpu.VMEM)
    packet = (n, 3 if wide else 2, rows, lanes)
    dma = pltpu.SemaphoreType.DMA
    return pl.pallas_call(
        functools.partial(exchange_kernel, n, n_prod, slices, loads, wide),
        out_shape=(
            jax.ShapeDtypeStruct(packet, F32),
            jax.ShapeDtypeStruct((2, 2, columns, lanes), F32),
            jax.ShapeDtypeStruct((8 + span, lanes), F32),
            jax.ShapeDtypeStruct((4 * span, 3 * span), jnp.bfloat16),
            jax.ShapeDtypeStruct((6, span, lanes), F32),
        ),
        in_specs=[smem, smem, smem, pl.BlockSpec(memory_space=pl.ANY)],
        out_specs=(vmem,) * 5,
        scratch_shapes=[
            pltpu.VMEM(sales.shape, F32),
            pltpu.VMEM((slices,) + packet[1:], F32),
            pltpu.VMEM(packet, F32),
            pltpu.VMEM(packet, F32),
            pltpu.VMEM((2, 2, columns, lanes), F32),
            pltpu.VMEM((n, 1, lanes), F32),
            pltpu.VMEM((n_prod, 8 + span, lanes), F32),
            dma((loads,)), dma((n,)), dma((n,)), dma((n,)), dma((n,)), dma((n,)), dma((n,)),
            dma((n_prod,)), dma((n_prod,)), dma((2, 2)), dma((2, 2)),
        ],
        compiler_params=pltpu.CompilerParams(collective_id=0, has_side_effects=True),
        name="exchange",
    )(week, month, year, sales)


def split3(value):
    high = value.astype(jnp.bfloat16)
    rest = value - high.astype(F32)
    middle = rest.astype(jnp.bfloat16)
    low = (rest - middle.astype(F32)).astype(jnp.bfloat16)
    return jnp.concatenate([high, middle, low], axis=-2)


def apply_kernel(
    wide, x, carry, near, meta, mixer, gains,
    run_out, week_out, month_out, year_out, rollup,
):
    _, span, lanes = x.shape
    groups, _, rows, _ = carry.shape

    @pl.when(pl.program_id(0) == 0)
    def _():
        mixed = jnp.dot(mixer[...], split3(meta[8 : 8 + span]), preferred_element_type=F32)
        rollup[0] = mixed[0:span] + meta[0:1]
        rollup[1] = mixed[span : 2 * span] + meta[3:4] * gains[0] + meta[5:6] * gains[1]
        rollup[2] = mixed[2 * span : 3 * span] + meta[4:5] * gains[2] + meta[6:7] * gains[3]
        rollup[3] = mixed[3 * span : 4 * span] + meta[1:2] * gains[4] + meta[2:3] * gains[5]

    def group(g, nothing):
        base = pl.multiple_of(g * rows, rows)
        at = pl.ds(base, rows)
        left_w, left_m = near[0, 0, at], near[0, 1, at]
        right_w, right_m = near[1, 0, at], near[1, 1, at]
        start = carry[g, 0]
        year_l, year_r = carry[g, 1 if wide else 0], carry[g, 2 if wide else 1]
        for r in range(0, rows, 2):
            parts = split3(x[pl.ds(base + r, 2)])
            both = jnp.concatenate([parts[0], parts[1]], axis=1)
            mixed = jnp.dot(mixer[...], both, preferred_element_type=F32)
            for j in range(2):
                q = r + j
                row = slice(q, q + 1)
                own = mixed[:, j * lanes : (j + 1) * lanes]
                run_out[base + q] = own[0:span] + start[row]
                week_out[base + q] = (
                    own[span : 2 * span] + left_w[row] * gains[0] + right_w[row] * gains[1]
                )
                month_out[base + q] = (
                    own[2 * span : 3 * span] + left_m[row] * gains[2] + right_m[row] * gains[3]
                )
                year_out[base + q] = (
                    own[3 * span : 4 * span] + year_l[row] * gains[4] + year_r[row] * gains[5]
                )
        return nothing

    lax.fori_loop(0, groups, group, 0, unroll=groups <= 2)


def apply(slices, wide, sales, carry, near, meta, mixer, gains):
    columns, span, lanes = sales.shape
    rows = columns // slices
    steps = 8 if slices % 8 == 0 else 1
    block = columns // steps
    cube = pl.BlockSpec((block, span, lanes), lambda i: (i, 0, 0))
    cube_shape = jax.ShapeDtypeStruct(sales.shape, F32)
    return pl.pallas_call(
        functools.partial(apply_kernel, wide),
        grid=(steps,),
        out_shape=(cube_shape,) * 4 + (jax.ShapeDtypeStruct((4, span, lanes), F32),),
        in_specs=[
            cube,
            pl.BlockSpec((slices // steps, carry.shape[1], rows, lanes), lambda i: (i, 0, 0, 0)),
            pl.BlockSpec((2, 2, block, lanes), lambda i: (0, 0, i, 0)),
            pl.BlockSpec(meta.shape, lambda i: (0, 0)),
            pl.BlockSpec(mixer.shape, lambda i: (0, 0)),
            pl.BlockSpec(gains.shape, lambda i: (0, 0, 0)),
        ],
        out_specs=(cube,) * 4 + (pl.BlockSpec((4, span, lanes), lambda i: (0, 0, 0)),),
        compiler_params=pltpu.CompilerParams(dimension_semantics=("arbitrary",)),
        name="apply",
    )(sales, carry, near, meta, mixer, gains)


def solution(mesh):
    n, n_prod = mesh.shape["date"], mesh.shape["prod"]

    def local(sales, week, month, year):
        slices = min(n, sales.shape[0] // 8)
        wide = n * sales.shape[1] // 300 + 1 > 2
        passed = exchange(n, n_prod, slices, wide, week, month, year, sales)
        return apply(slices, wide, sales, *passed)

    return jax.shard_map(
        local,
        mesh=mesh,
        in_specs=(P("prod", "date", None), P("date"), P("date"), P("date")),
        out_specs=(P("prod", "date", None),) * 4 + (P(None, "date", None),),
        check_vma=False,
    )
```

```python
import functools

import jax
import jax.numpy as jnp
from jax import lax
from jax.experimental import pallas as pl
from jax.experimental.pallas import tpu as pltpu
from jax.sharding import PartitionSpec as P

MESH = pl.DeviceIdType.MESH
F32 = jnp.float32


def id_column(ids, span, lanes):
    where = lax.broadcasted_iota(jnp.int32, (span, lanes), 0)
    column = jnp.zeros((span, lanes), jnp.int32)
    for t in range(span):
        column = jnp.where(where == t, ids[t], column)
    return column


def id_row(ids, span, lanes):
    where = lax.broadcasted_iota(jnp.int32, (span, lanes), 1) % span
    row = jnp.zeros((span, lanes), jnp.int32)
    for t in range(span):
        row = jnp.where(where == t, ids[t], row)
    return row


def edge_masks(ids, span, lanes):
    column = id_column(ids, span, lanes)
    return (column == ids[0]).astype(F32), (column == ids[span - 1]).astype(F32)


def stack_rows(values, rows, lanes):
    where = lax.broadcasted_iota(jnp.int32, (rows, lanes), 0)
    tile = jnp.zeros((rows, lanes), F32)
    for i, value in enumerate(values):
        tile = jnp.where(where == i, value, tile)
    return tile


def exchange_kernel(
    n, n_prod, slices, loads, wide,
    week_hbm, month_hbm, year_hbm, x_hbm,
    carry, near, meta_hbm, mixer_hbm, gains_hbm,
    week, month, year, meta, mixer, gains,
    x, send1, recv1, send2, edges, seen, summed, parts,
    ids_sem, out_sem, sum_s, sum_r, load_sem, id_s, id_r, s1_sem, r1_sem, s2_sem, r2_sem, sib_s, sib_r, near_s, near_r,
):
    me = lax.axis_index("date")
    core = lax.axis_index("prod")
    columns, span, lanes = x.shape
    rows = columns // slices
    chunk = columns // loads
    last = span - 1
    loaded = [
        pltpu.make_async_copy(
            x_hbm.at[pl.ds(i * chunk, chunk)], x.at[pl.ds(i * chunk, chunk)], load_sem.at[i]
        )
        for i in range(loads)
    ]
    for copy in loaded:
        copy.start()
    fetched = [
        pltpu.make_async_copy(source, target, ids_sem.at[i])
        for i, (source, target) in enumerate(
            ((year_hbm, year), (week_hbm, week), (month_hbm, month))
        )
    ]
    for copy in fetched:
        copy.start()
    barrier = pltpu.get_barrier_semaphore()
    for d in range(1, n):
        pl.semaphore_signal(
            barrier, inc=1, device_id=(lax.rem(me + d, n), core), device_id_type=MESH
        )
    for d in range(1, n_prod):
        pl.semaphore_signal(
            barrier, inc=1, device_id=(me, lax.rem(core + d, n_prod)), device_id_type=MESH
        )
    for copy in fetched:
        copy.wait()
    lane = lax.broadcasted_iota(jnp.int32, (1, lanes), 1)
    ids = jnp.zeros((1, lanes), F32)
    for i, v in enumerate((year[0], year[last], week[0], week[last], month[0], month[last])):
        ids = jnp.where(lane == i, v.astype(F32), ids)
    seen[me] = ids
    head_y, tail_y = edge_masks(year, span, lanes)

    def outer_sums(s, total):
        block = x[pl.ds(pl.multiple_of(s * rows, rows), rows)]
        send1[s, 0] = jnp.sum(block * head_y[None], axis=1)
        send1[s, 1] = jnp.sum(block * tail_y[None], axis=1)
        if wide:
            send1[s, 2] = jnp.sum(block, axis=1)
        return total + jnp.sum(block, axis=0)

    total = jnp.zeros((span, lanes), F32)
    per_load = slices // loads
    for i in range(loads):
        loaded[i].wait()
        total = lax.fori_loop(i * per_load, (i + 1) * per_load, outer_sums, total)
    recv1[me] = send1[lax.rem(me, slices)]
    pl.semaphore_wait(barrier, n - 1 + n_prod - 1)

    def to_all(source, target, send_sem, recv_sem):
        copies = []
        for d in range(1, n):
            peer = lax.rem(me + d, n)
            copy = pltpu.make_async_remote_copy(
                src_ref=source(peer), dst_ref=target.at[me],
                send_sem=send_sem.at[peer], recv_sem=recv_sem.at[me],
                device_id=(peer, core), device_id_type=MESH,
            )
            copy.start()
            copies.append(copy)
        return copies

    def arrived(target, send_sem, recv_sem):
        for d in range(1, n):
            peer = lax.rem(me + d, n)
            pltpu.make_async_remote_copy(
                src_ref=target.at[me], dst_ref=target.at[peer],
                send_sem=send_sem.at[peer], recv_sem=recv_sem.at[peer],
                device_id=(peer, core), device_id_type=MESH,
            ).wait_recv()

    sent = to_all(lambda peer: seen.at[me], seen, id_s, id_r)
    sent += to_all(lambda peer: send1.at[lax.rem(peer, slices)], recv1, s1_sem, r1_sem)

    head_w, tail_w = edge_masks(week, span, lanes)
    head_m, tail_m = edge_masks(month, span, lanes)
    summed[me] = stack_rows(
        [jnp.sum(total, axis=0, keepdims=True)]
        + [
            jnp.sum(total * m, axis=0, keepdims=True)
            for m in (head_y, tail_y, head_w, tail_w, head_m, tail_m)
        ],
        8, lanes,
    )
    left, right = lax.rem(me + n - 1, n), lax.rem(me + 1, n)

    def edge_sums(level, head, tail):
        def inner_sums(s, nothing):
            at = pl.ds(pl.multiple_of(s * rows, rows), rows)
            block = x[at]
            edges[0, level, at] = jnp.sum(block * tail[None], axis=1)
            edges[1, level, at] = jnp.sum(block * head[None], axis=1)
            return nothing

        lax.fori_loop(0, slices, inner_sums, 0)

    def edge_send(side, level):
        copy = pltpu.make_async_remote_copy(
            src_ref=edges.at[side, level], dst_ref=near.at[side, level],
            send_sem=near_s.at[side, level], recv_sem=near_r.at[side, level],
            device_id=((right, left)[side], core), device_id_type=MESH,
        )
        copy.start()
        return copy

    edge_sums(0, head_w, tail_w)
    sent += to_all(lambda peer: summed.at[me], summed, sum_s, sum_r)
    beside = [edge_send(0, 0), edge_send(1, 0)]
    edge_sums(1, head_m, tail_m)
    beside.append(edge_send(0, 1))

    sub = lax.broadcasted_iota(jnp.int32, (span, 3 * span), 0)
    place = lax.broadcasted_iota(jnp.int32, (span, 3 * span), 1) % span
    mixer[0:span] = jnp.where(place <= sub, 1.0, 0.0).astype(mixer.dtype)
    for k, level in enumerate((week, month, year)):
        same = id_column(level, span, 3 * span) == id_row(level, span, 3 * span)
        mixer[(k + 1) * span : (k + 2) * span] = jnp.where(same, 1.0, 0.0).astype(mixer.dtype)

    arrived(seen, id_s, id_r)
    low = [jnp.broadcast_to(seen[b][:, 0:1], (rows, lanes)) for b in range(n)]
    top = [jnp.broadcast_to(seen[b][:, 1:2], (rows, lanes)) for b in range(n)]
    arrived(recv1, s1_sem, r1_sem)
    zero = jnp.zeros((rows, lanes), F32)
    running, into = zero, zero
    brought = []
    for b in range(n):
        send2[b, 0] = running
        brought.append(into)
        if wide:
            send2[b, 1] = into
        if b + 1 < n:
            head, tail = recv1[b, 0], recv1[b, 1]
            one = low[b] == top[b]
            running = running + (recv1[b, 2] if wide else head + jnp.where(one, 0.0, tail))
            into = jnp.where(top[b] == low[b + 1], tail + jnp.where(one, into, 0.0), 0.0)
    back = zero
    for b in reversed(range(n)):
        one = low[b] == top[b]
        if wide:
            send2[b, 2] = back
        else:
            send2[b, 1] = back + jnp.where(one, brought[b], 0.0)
        if b > 0:
            held = recv1[b, 0] + jnp.where(one, back, 0.0)
            back = jnp.where(top[b - 1] == low[b], held, 0.0)
    sent += to_all(lambda peer: send2.at[peer], carry, s2_sem, r2_sem)
    beside.append(edge_send(1, 1))
    kept = pltpu.make_async_copy(send2.at[me], carry.at[me], out_sem.at[0])
    kept.start()

    def gain(there, lane_seen, own, where):
        value = jnp.broadcast_to(seen[there][:, lane_seen : lane_seen + 1], (1, lanes))
        return jnp.where(jnp.logical_and(value == own.astype(F32), where), 1.0, 0.0)

    gains[0] = head_w * gain(left, 3, week[0], me > 0)
    gains[1] = tail_w * gain(right, 2, week[last], me < n - 1)
    gains[2] = head_m * gain(left, 5, month[0], me > 0)
    gains[3] = tail_m * gain(right, 4, month[last], me < n - 1)
    gains[4] = head_y if wide else head_y * jnp.where(year[0] == year[last], 0.0, 1.0)
    gains[5] = tail_y
    leaving = [
        pltpu.make_async_copy(mixer, mixer_hbm, out_sem.at[1]),
        pltpu.make_async_copy(gains, gains_hbm, out_sem.at[2]),
    ]
    for copy in leaving:
        copy.start()

    arrived(summed, sum_s, sum_r)
    run_sum = jnp.zeros((1, lanes), F32)
    in_sum, back_sum = run_sum, run_sum
    low_me, top_me = low[0][0:1] * 0.0, top[0][0:1] * 0.0
    low_me = low_me + year[0].astype(F32)
    top_me = top_me + year[last].astype(F32)
    for b in range(n):
        tile = summed[b]
        run_sum = run_sum + jnp.where(b < me, tile[0:1], 0.0)
        inside = jnp.logical_and(top[b][0:1] == low_me, b < me)
        in_sum = in_sum + jnp.where(inside, tile[2:3], 0.0)
        inside = jnp.logical_and(low[b][0:1] == top_me, b > me)
        back_sum = back_sum + jnp.where(inside, tile[1:2], 0.0)
    if wide:
        first_sum, last_sum = in_sum, back_sum
    else:
        first_sum = run_sum
        last_sum = back_sum + jnp.where(low_me == top_me, in_sum, 0.0)
    from_left, from_right = summed[left], summed[right]
    parts[core, 0:8] = stack_rows(
        [
            run_sum, first_sum, last_sum,
            from_left[4:5], from_left[6:7], from_right[3:4], from_right[5:6],
        ],
        8, lanes,
    )
    parts[core, 8 : 8 + span] = total
    shared = []
    for d in range(1, n_prod):
        peer = lax.rem(core + d, n_prod)
        copy = pltpu.make_async_remote_copy(
            src_ref=parts.at[core], dst_ref=parts.at[core],
            send_sem=sib_s.at[peer], recv_sem=sib_r.at[core],
            device_id=(me, peer), device_id_type=MESH,
        )
        copy.start()
        shared.append(copy)
    for d in range(1, n_prod):
        peer = lax.rem(core + d, n_prod)
        pltpu.make_async_remote_copy(
            src_ref=parts.at[core], dst_ref=parts.at[peer],
            send_sem=sib_s.at[peer], recv_sem=sib_r.at[peer],
            device_id=(me, peer), device_id_type=MESH,
        ).wait_recv()
    whole = parts[0]
    for i in range(1, n_prod):
        whole = whole + parts[i]
    meta[...] = whole
    last_out = pltpu.make_async_copy(meta, meta_hbm, out_sem.at[3])
    last_out.start()
    for copy in sent + beside + shared:
        copy.wait_send()
    kept.wait()
    for copy in leaving:
        copy.wait()
    for copy in beside:
        copy.wait_recv()
    arrived(carry, s2_sem, r2_sem)
    last_out.wait()


def exchange(n, n_prod, slices, wide, week, month, year, sales):
    columns, span, lanes = sales.shape
    rows = columns // slices
    loads = 4 if slices % 4 == 0 else 1
    anywhere = pl.BlockSpec(memory_space=pl.ANY)
    packet = (n, 3 if wide else 2, rows, lanes)
    dma = pltpu.SemaphoreType.DMA
    return pl.pallas_call(
        functools.partial(exchange_kernel, n, n_prod, slices, loads, wide),
        out_shape=(
            jax.ShapeDtypeStruct(packet, F32),
            jax.ShapeDtypeStruct((2, 2, columns, lanes), F32),
            jax.ShapeDtypeStruct((8 + span, lanes), F32),
            jax.ShapeDtypeStruct((4 * span, 3 * span), jnp.bfloat16),
            jax.ShapeDtypeStruct((6, span, lanes), F32),
        ),
        in_specs=[anywhere] * 4,
        out_specs=(anywhere,) * 5,
        scratch_shapes=[
            pltpu.SMEM((span,), jnp.int32),
            pltpu.SMEM((span,), jnp.int32),
            pltpu.SMEM((span,), jnp.int32),
            pltpu.VMEM((8 + span, lanes), F32),
            pltpu.VMEM((4 * span, 3 * span), jnp.bfloat16),
            pltpu.VMEM((6, span, lanes), F32),
            pltpu.VMEM(sales.shape, F32),
            pltpu.VMEM((slices,) + packet[1:], F32),
            pltpu.VMEM(packet, F32),
            pltpu.VMEM(packet, F32),
            pltpu.VMEM((2, 2, columns, lanes), F32),
            pltpu.VMEM((n, 1, lanes), F32),
            pltpu.VMEM((n, 8, lanes), F32),
            pltpu.VMEM((n_prod, 8 + span, lanes), F32),
            dma((3,)), dma((4,)), dma((n,)), dma((n,)), dma((loads,)), dma((n,)), dma((n,)), dma((n,)), dma((n,)), dma((n,)), dma((n,)),
            dma((n_prod,)), dma((n_prod,)), dma((2, 2)), dma((2, 2)),
        ],
        compiler_params=pltpu.CompilerParams(collective_id=0, has_side_effects=True),
        name="exchange",
    )(week, month, year, sales)


def split3(value):
    high = value.astype(jnp.bfloat16)
    rest = value - high.astype(F32)
    middle = rest.astype(jnp.bfloat16)
    low = (rest - middle.astype(F32)).astype(jnp.bfloat16)
    return jnp.concatenate([high, middle, low], axis=-2)


def apply_kernel(
    wide, steps, x_hbm, carry_hbm, near_hbm, meta_hbm, mixer_hbm, gains_hbm,
    run_hbm, week_hbm, month_hbm, year_hbm, rollup_hbm,
    x, carry, near, meta, mixer, gains, run_out, week_out, month_out, year_out, rollup,
    x_sem, in_sem, out_sem, rollup_sem,
):
    columns, span, lanes = x.shape
    groups, _, rows, _ = carry.shape
    per_step = groups // steps
    block = columns // steps
    small = [
        pltpu.make_async_copy(source, target, in_sem.at[i])
        for i, (source, target) in enumerate(
            (
                (mixer_hbm, mixer), (gains_hbm, gains),
                (carry_hbm.at[pl.ds(0, groups)], carry), (near_hbm, near), (meta_hbm, meta),
            )
        )
    ]
    pieces = [pl.ds(i * block, block) for i in range(steps)]
    loads = [
        pltpu.make_async_copy(x_hbm.at[at], x.at[at], x_sem.at[i]) for i, at in enumerate(pieces)
    ]
    loads[0].start()
    for copy in small:
        copy.start()
    for copy in loads[1:]:
        copy.start()
    for copy in small:
        copy.wait()

    def group(g, nothing):
        base = pl.multiple_of(g * rows, rows)
        at = pl.ds(base, rows)
        left_w, left_m = near[0, 0, at], near[0, 1, at]
        right_w, right_m = near[1, 0, at], near[1, 1, at]
        start = carry[g, 0]
        year_l, year_r = carry[g, 1 if wide else 0], carry[g, 2 if wide else 1]
        for r in range(0, rows, 2):
            parts = split3(x[pl.ds(base + r, 2)])
            both = jnp.concatenate([parts[0], parts[1]], axis=1)
            mixed = jnp.dot(mixer[...], both, preferred_element_type=F32)
            for j in range(2):
                q = r + j
                row = slice(q, q + 1)
                own = mixed[:, j * lanes : (j + 1) * lanes]
                run_out[base + q] = own[0:span] + start[row]
                week_out[base + q] = (
                    own[span : 2 * span] + left_w[row] * gains[0] + right_w[row] * gains[1]
                )
                month_out[base + q] = (
                    own[2 * span : 3 * span] + left_m[row] * gains[2] + right_m[row] * gains[3]
                )
                year_out[base + q] = (
                    own[3 * span : 4 * span] + year_l[row] * gains[4] + year_r[row] * gains[5]
                )
        return nothing

    stores = []
    for i, at in enumerate(pieces):
        loads[i].wait()
        lax.fori_loop(i * per_step, (i + 1) * per_step, group, 0)
        for k, (source, target) in enumerate(
            (
                (run_out, run_hbm), (week_out, week_hbm),
                (month_out, month_hbm), (year_out, year_hbm),
            )
        ):
            copy = pltpu.make_async_copy(source.at[at], target.at[at], out_sem.at[i, k])
            copy.start()
            stores.append(copy)
        if i == 0:
            mixed = jnp.dot(mixer[...], split3(meta[8 : 8 + span]), preferred_element_type=F32)
            rollup[0] = mixed[0:span] + meta[0:1]
            rollup[1] = mixed[span : 2 * span] + meta[3:4] * gains[0] + meta[5:6] * gains[1]
            rollup[2] = mixed[2 * span : 3 * span] + meta[4:5] * gains[2] + meta[6:7] * gains[3]
            rollup[3] = mixed[3 * span : 4 * span] + meta[1:2] * gains[4] + meta[2:3] * gains[5]
            copy = pltpu.make_async_copy(rollup, rollup_hbm, rollup_sem.at[0])
            copy.start()
            stores.append(copy)
    for copy in stores:
        copy.wait()


def apply(slices, wide, sales, carry, near, meta, mixer, gains):
    span, lanes = sales.shape[1:]
    steps = 8 if slices % 8 == 0 else 1
    anywhere = pl.BlockSpec(memory_space=pl.ANY)
    cube_shape = jax.ShapeDtypeStruct(sales.shape, F32)
    cube = pltpu.VMEM(sales.shape, F32)
    dma = pltpu.SemaphoreType.DMA
    return pl.pallas_call(
        functools.partial(apply_kernel, wide, steps),
        out_shape=(cube_shape,) * 4 + (jax.ShapeDtypeStruct((4, span, lanes), F32),),
        in_specs=[anywhere] * 6,
        out_specs=(anywhere,) * 5,
        scratch_shapes=[
            cube,
            pltpu.VMEM((slices,) + carry.shape[1:], F32),
            pltpu.VMEM(near.shape, F32),
            pltpu.VMEM(meta.shape, F32),
            pltpu.VMEM(mixer.shape, mixer.dtype),
            pltpu.VMEM(gains.shape, F32),
            cube, cube, cube, cube,
            pltpu.VMEM((4, span, lanes), F32),
            dma((steps,)), dma((5,)), dma((steps, 4)), dma((1,)),
        ],
        name="apply",
    )(sales, carry, near, meta, mixer, gains)


def solution(mesh):
    n, n_prod = mesh.shape["date"], mesh.shape["prod"]

    def local(sales, week, month, year):
        slices = min(n, sales.shape[0] // 8)
        wide = n * sales.shape[1] // 300 + 1 > 2
        passed = exchange(n, n_prod, slices, wide, week, month, year, sales)
        return apply(slices, wide, sales, *passed)

    return jax.shard_map(
        local,
        mesh=mesh,
        in_specs=(P("prod", "date", None), P("date"), P("date"), P("date")),
        out_specs=(P("prod", "date", None),) * 4 + (P(None, "date", None),),
        check_vma=False,
    )
```

```python
import functools

import jax
import jax.numpy as jnp
from jax import lax
from jax.experimental import pallas as pl
from jax.experimental.pallas import tpu as pltpu
from jax.sharding import PartitionSpec as P

MESH = pl.DeviceIdType.MESH
F32 = jnp.float32


def id_column(ids, span, lanes):
    where = lax.broadcasted_iota(jnp.int32, (span, lanes), 0)
    column = jnp.zeros((span, lanes), jnp.int32)
    for t in range(span):
        column = jnp.where(where == t, ids[t], column)
    return column


def id_row(ids, span, lanes):
    where = lax.broadcasted_iota(jnp.int32, (span, lanes), 1) % span
    row = jnp.zeros((span, lanes), jnp.int32)
    for t in range(span):
        row = jnp.where(where == t, ids[t], row)
    return row


def edge_masks(ids, span, lanes):
    column = id_column(ids, span, lanes)
    return (column == ids[0]).astype(F32), (column == ids[span - 1]).astype(F32)


def stack_rows(values, rows, lanes):
    where = lax.broadcasted_iota(jnp.int32, (rows, lanes), 0)
    tile = jnp.zeros((rows, lanes), F32)
    for i, value in enumerate(values):
        tile = jnp.where(where == i, value, tile)
    return tile


def exchange_kernel(
    n, n_prod, slices, loads, wide,
    week_hbm, month_hbm, year_hbm, x_hbm,
    carry, near, meta_hbm, mixer_hbm, gains_hbm,
    week, month, year, meta, mixer, gains,
    x, send1, recv1, send2, edges, seen, summed, parts,
    ids_sem, out_sem, sum_s, sum_r, load_sem, id_s, id_r, s1_sem, r1_sem, s2_sem, r2_sem, sib_s, sib_r, near_s, near_r,
):
    me = lax.axis_index("date")
    core = lax.axis_index("prod")
    columns, span, lanes = x.shape
    rows = columns // slices
    chunk = columns // loads
    last = span - 1
    loaded = [
        pltpu.make_async_copy(
            x_hbm.at[pl.ds(i * chunk, chunk)], x.at[pl.ds(i * chunk, chunk)], load_sem.at[i]
        )
        for i in range(loads)
    ]
    for copy in loaded:
        copy.start()
    fetched = [
        pltpu.make_async_copy(source, target, ids_sem.at[i])
        for i, (source, target) in enumerate(
            ((year_hbm, year), (week_hbm, week), (month_hbm, month))
        )
    ]
    for copy in fetched:
        copy.start()
    barrier = pltpu.get_barrier_semaphore()
    for d in range(1, n):
        pl.semaphore_signal(
            barrier, inc=1, device_id=(lax.rem(me + d, n), core), device_id_type=MESH
        )
    for d in range(1, n_prod):
        pl.semaphore_signal(
            barrier, inc=1, device_id=(me, lax.rem(core + d, n_prod)), device_id_type=MESH
        )
    for copy in fetched:
        copy.wait()
    lane = lax.broadcasted_iota(jnp.int32, (1, lanes), 1)
    ids = jnp.zeros((1, lanes), F32)
    for i, v in enumerate((year[0], year[last], week[0], week[last], month[0], month[last])):
        ids = jnp.where(lane == i, v.astype(F32), ids)
    seen[me] = ids
    head_y, tail_y = edge_masks(year, span, lanes)

    def outer_sums(s, total):
        block = x[pl.ds(pl.multiple_of(s * rows, rows), rows)]
        send1[s, 0] = jnp.sum(block * head_y[None], axis=1)
        send1[s, 1] = jnp.sum(block * tail_y[None], axis=1)
        if wide:
            send1[s, 2] = jnp.sum(block, axis=1)
        return total + jnp.sum(block, axis=0)

    total = jnp.zeros((span, lanes), F32)
    per_load = slices // loads
    for i in range(loads):
        loaded[i].wait()
        total = lax.fori_loop(i * per_load, (i + 1) * per_load, outer_sums, total)
    recv1[me] = send1[lax.rem(me, slices)]
    pl.semaphore_wait(barrier, n - 1 + n_prod - 1)

    def to_all(source, target, send_sem, recv_sem):
        copies = []
        for d in sorted(range(1, n), key=lambda d: -min(d, n - d)):
            peer = lax.rem(me + d, n)
            copy = pltpu.make_async_remote_copy(
                src_ref=source(peer), dst_ref=target.at[me],
                send_sem=send_sem.at[peer], recv_sem=recv_sem.at[me],
                device_id=(peer, core), device_id_type=MESH,
            )
            copy.start()
            copies.append(copy)
        return copies

    def arrived(target, send_sem, recv_sem):
        for d in range(1, n):
            peer = lax.rem(me + d, n)
            pltpu.make_async_remote_copy(
                src_ref=target.at[me], dst_ref=target.at[peer],
                send_sem=send_sem.at[peer], recv_sem=recv_sem.at[peer],
                device_id=(peer, core), device_id_type=MESH,
            ).wait_recv()

    sent = to_all(lambda peer: seen.at[me], seen, id_s, id_r)
    sent += to_all(lambda peer: send1.at[lax.rem(peer, slices)], recv1, s1_sem, r1_sem)

    head_w, tail_w = edge_masks(week, span, lanes)
    head_m, tail_m = edge_masks(month, span, lanes)
    summed[me] = stack_rows(
        [jnp.sum(total, axis=0, keepdims=True)]
        + [
            jnp.sum(total * m, axis=0, keepdims=True)
            for m in (head_y, tail_y, head_w, tail_w, head_m, tail_m)
        ],
        8, lanes,
    )
    left, right = lax.rem(me + n - 1, n), lax.rem(me + 1, n)

    def edge_sums(level, head, tail):
        def inner_sums(s, nothing):
            at = pl.ds(pl.multiple_of(s * rows, rows), rows)
            block = x[at]
            edges[0, level, at] = jnp.sum(block * tail[None], axis=1)
            edges[1, level, at] = jnp.sum(block * head[None], axis=1)
            return nothing

        lax.fori_loop(0, slices, inner_sums, 0)

    linked = (me < n - 1, me > 0)

    def edge_copy(side, level):
        return pltpu.make_async_remote_copy(
            src_ref=edges.at[side, level], dst_ref=near.at[side, level],
            send_sem=near_s.at[side, level], recv_sem=near_r.at[side, level],
            device_id=((right, left)[side], core), device_id_type=MESH,
        )

    def edge_send(side, level):
        @pl.when(linked[side])
        def _():
            edge_copy(side, level).start()

        @pl.when(jnp.logical_not(linked[side]))
        def _():
            pltpu.make_async_copy(
                edges.at[side, level], near.at[1 - side, level], near_r.at[1 - side, level]
            ).start()

    edge_sums(0, head_w, tail_w)
    sent += to_all(lambda peer: summed.at[me], summed, sum_s, sum_r)
    edge_send(0, 0)
    edge_send(1, 0)
    edge_sums(1, head_m, tail_m)
    edge_send(0, 1)

    sub = lax.broadcasted_iota(jnp.int32, (span, 3 * span), 0)
    place = lax.broadcasted_iota(jnp.int32, (span, 3 * span), 1) % span
    mixer[0:span] = jnp.where(place <= sub, 1.0, 0.0).astype(mixer.dtype)
    for k, level in enumerate((week, month, year)):
        same = id_column(level, span, 3 * span) == id_row(level, span, 3 * span)
        mixer[(k + 1) * span : (k + 2) * span] = jnp.where(same, 1.0, 0.0).astype(mixer.dtype)

    arrived(seen, id_s, id_r)
    low = [jnp.broadcast_to(seen[b][:, 0:1], (rows, lanes)) for b in range(n)]
    top = [jnp.broadcast_to(seen[b][:, 1:2], (rows, lanes)) for b in range(n)]
    arrived(recv1, s1_sem, r1_sem)
    zero = jnp.zeros((rows, lanes), F32)
    running, into = zero, zero
    brought = []
    for b in range(n):
        send2[b, 0] = running
        brought.append(into)
        if wide:
            send2[b, 1] = into
        if b + 1 < n:
            head, tail = recv1[b, 0], recv1[b, 1]
            one = low[b] == top[b]
            running = running + (recv1[b, 2] if wide else head + jnp.where(one, 0.0, tail))
            into = jnp.where(top[b] == low[b + 1], tail + jnp.where(one, into, 0.0), 0.0)
    back = zero
    for b in reversed(range(n)):
        one = low[b] == top[b]
        if wide:
            send2[b, 2] = back
        else:
            send2[b, 1] = back + jnp.where(one, brought[b], 0.0)
        if b > 0:
            held = recv1[b, 0] + jnp.where(one, back, 0.0)
            back = jnp.where(top[b - 1] == low[b], held, 0.0)
    sent += to_all(lambda peer: send2.at[peer], carry, s2_sem, r2_sem)
    edge_send(1, 1)
    kept = pltpu.make_async_copy(send2.at[me], carry.at[me], out_sem.at[0])
    kept.start()

    def gain(there, lane_seen, own, where):
        value = jnp.broadcast_to(seen[there][:, lane_seen : lane_seen + 1], (1, lanes))
        return jnp.where(jnp.logical_and(value == own.astype(F32), where), 1.0, 0.0)

    gains[0] = head_w * gain(left, 3, week[0], me > 0)
    gains[1] = tail_w * gain(right, 2, week[last], me < n - 1)
    gains[2] = head_m * gain(left, 5, month[0], me > 0)
    gains[3] = tail_m * gain(right, 4, month[last], me < n - 1)
    gains[4] = head_y if wide else head_y * jnp.where(year[0] == year[last], 0.0, 1.0)
    gains[5] = tail_y
    leaving = [
        pltpu.make_async_copy(mixer, mixer_hbm, out_sem.at[1]),
        pltpu.make_async_copy(gains, gains_hbm, out_sem.at[2]),
    ]
    for copy in leaving:
        copy.start()

    arrived(summed, sum_s, sum_r)
    run_sum = jnp.zeros((1, lanes), F32)
    in_sum, back_sum = run_sum, run_sum
    low_me, top_me = low[0][0:1] * 0.0, top[0][0:1] * 0.0
    low_me = low_me + year[0].astype(F32)
    top_me = top_me + year[last].astype(F32)
    for b in range(n):
        tile = summed[b]
        run_sum = run_sum + jnp.where(b < me, tile[0:1], 0.0)
        inside = jnp.logical_and(top[b][0:1] == low_me, b < me)
        in_sum = in_sum + jnp.where(inside, tile[2:3], 0.0)
        inside = jnp.logical_and(low[b][0:1] == top_me, b > me)
        back_sum = back_sum + jnp.where(inside, tile[1:2], 0.0)
    if wide:
        first_sum, last_sum = in_sum, back_sum
    else:
        first_sum = run_sum
        last_sum = back_sum + jnp.where(low_me == top_me, in_sum, 0.0)
    from_left, from_right = summed[left], summed[right]
    parts[core, 0:8] = stack_rows(
        [
            run_sum, first_sum, last_sum,
            from_left[4:5], from_left[6:7], from_right[3:4], from_right[5:6],
        ],
        8, lanes,
    )
    parts[core, 8 : 8 + span] = total
    shared = []
    for d in range(1, n_prod):
        peer = lax.rem(core + d, n_prod)
        copy = pltpu.make_async_remote_copy(
            src_ref=parts.at[core], dst_ref=parts.at[core],
            send_sem=sib_s.at[peer], recv_sem=sib_r.at[core],
            device_id=(me, peer), device_id_type=MESH,
        )
        copy.start()
        shared.append(copy)
    for d in range(1, n_prod):
        peer = lax.rem(core + d, n_prod)
        pltpu.make_async_remote_copy(
            src_ref=parts.at[core], dst_ref=parts.at[peer],
            send_sem=sib_s.at[peer], recv_sem=sib_r.at[peer],
            device_id=(me, peer), device_id_type=MESH,
        ).wait_recv()
    whole = parts[0]
    for i in range(1, n_prod):
        whole = whole + parts[i]
    meta[...] = whole
    last_out = pltpu.make_async_copy(meta, meta_hbm, out_sem.at[3])
    last_out.start()
    for copy in sent + shared:
        copy.wait_send()
    kept.wait()
    for copy in leaving:
        copy.wait()
    for side in range(2):
        for level in range(2):
            edge_copy(side, level).wait_recv()

            @pl.when(linked[side])
            def _():
                edge_copy(side, level).wait_send()

    arrived(carry, s2_sem, r2_sem)
    last_out.wait()


def exchange(n, n_prod, slices, wide, week, month, year, sales):
    columns, span, lanes = sales.shape
    rows = columns // slices
    loads = 4 if slices % 4 == 0 else 1
    anywhere = pl.BlockSpec(memory_space=pl.ANY)
    packet = (n, 3 if wide else 2, rows, lanes)
    dma = pltpu.SemaphoreType.DMA
    return pl.pallas_call(
        functools.partial(exchange_kernel, n, n_prod, slices, loads, wide),
        out_shape=(
            jax.ShapeDtypeStruct(packet, F32),
            jax.ShapeDtypeStruct((2, 2, columns, lanes), F32),
            jax.ShapeDtypeStruct((8 + span, lanes), F32),
            jax.ShapeDtypeStruct((4 * span, 3 * span), jnp.bfloat16),
            jax.ShapeDtypeStruct((6, span, lanes), F32),
        ),
        in_specs=[anywhere] * 4,
        out_specs=(anywhere,) * 5,
        scratch_shapes=[
            pltpu.SMEM((span,), jnp.int32),
            pltpu.SMEM((span,), jnp.int32),
            pltpu.SMEM((span,), jnp.int32),
            pltpu.VMEM((8 + span, lanes), F32),
            pltpu.VMEM((4 * span, 3 * span), jnp.bfloat16),
            pltpu.VMEM((6, span, lanes), F32),
            pltpu.VMEM(sales.shape, F32),
            pltpu.VMEM((slices,) + packet[1:], F32),
            pltpu.VMEM(packet, F32),
            pltpu.VMEM(packet, F32),
            pltpu.VMEM((2, 2, columns, lanes), F32),
            pltpu.VMEM((n, 1, lanes), F32),
            pltpu.VMEM((n, 8, lanes), F32),
            pltpu.VMEM((n_prod, 8 + span, lanes), F32),
            dma((3,)), dma((4,)), dma((n,)), dma((n,)), dma((loads,)), dma((n,)), dma((n,)), dma((n,)), dma((n,)), dma((n,)), dma((n,)),
            dma((n_prod,)), dma((n_prod,)), dma((2, 2)), dma((2, 2)),
        ],
        compiler_params=pltpu.CompilerParams(collective_id=0, has_side_effects=True),
        name="exchange",
    )(week, month, year, sales)


def split3(value):
    high = value.astype(jnp.bfloat16)
    rest = value - high.astype(F32)
    middle = rest.astype(jnp.bfloat16)
    low = (rest - middle.astype(F32)).astype(jnp.bfloat16)
    return jnp.concatenate([high, middle, low], axis=-2)


def apply_kernel(
    wide, steps, x_hbm, carry_hbm, near_hbm, meta_hbm, mixer_hbm, gains_hbm,
    run_hbm, week_hbm, month_hbm, year_hbm, rollup_hbm,
    x, carry, near, meta, mixer, gains, run_out, week_out, month_out, year_out, rollup,
    x_sem, in_sem, out_sem, rollup_sem,
):
    columns, span, lanes = x.shape
    groups, _, rows, _ = carry.shape
    per_step = groups // steps
    block = columns // steps
    small = [
        pltpu.make_async_copy(source, target, in_sem.at[i])
        for i, (source, target) in enumerate(
            (
                (mixer_hbm, mixer), (gains_hbm, gains),
                (carry_hbm.at[pl.ds(0, groups)], carry), (near_hbm, near), (meta_hbm, meta),
            )
        )
    ]
    pieces = [pl.ds(i * block, block) for i in range(steps)]
    loads = [
        pltpu.make_async_copy(x_hbm.at[at], x.at[at], x_sem.at[i]) for i, at in enumerate(pieces)
    ]
    loads[0].start()
    for copy in small:
        copy.start()
    for copy in loads[1:]:
        copy.start()
    for copy in small:
        copy.wait()

    def group(g, nothing):
        base = pl.multiple_of(g * rows, rows)
        at = pl.ds(base, rows)
        left_w, left_m = near[0, 0, at], near[0, 1, at]
        right_w, right_m = near[1, 0, at], near[1, 1, at]
        start = carry[g, 0]
        year_l, year_r = carry[g, 1 if wide else 0], carry[g, 2 if wide else 1]
        for r in range(0, rows, 2):
            parts = split3(x[pl.ds(base + r, 2)])
            both = jnp.concatenate([parts[0], parts[1]], axis=1)
            mixed = jnp.dot(mixer[...], both, preferred_element_type=F32)
            for j in range(2):
                q = r + j
                row = slice(q, q + 1)
                own = mixed[:, j * lanes : (j + 1) * lanes]
                run_out[base + q] = own[0:span] + start[row]
                week_out[base + q] = (
                    own[span : 2 * span] + left_w[row] * gains[0] + right_w[row] * gains[1]
                )
                month_out[base + q] = (
                    own[2 * span : 3 * span] + left_m[row] * gains[2] + right_m[row] * gains[3]
                )
                year_out[base + q] = (
                    own[3 * span : 4 * span] + year_l[row] * gains[4] + year_r[row] * gains[5]
                )
        return nothing

    stores = []
    for i, at in enumerate(pieces):
        loads[i].wait()
        lax.fori_loop(i * per_step, (i + 1) * per_step, group, 0, unroll=per_step <= 2)
        for k, (source, target) in enumerate(
            (
                (run_out, run_hbm), (week_out, week_hbm),
                (month_out, month_hbm), (year_out, year_hbm),
            )
        ):
            copy = pltpu.make_async_copy(source.at[at], target.at[at], out_sem.at[i, k])
            copy.start()
            stores.append(copy)
        if i == 0:
            mixed = jnp.dot(mixer[...], split3(meta[8 : 8 + span]), preferred_element_type=F32)
            rollup[0] = mixed[0:span] + meta[0:1]
            rollup[1] = mixed[span : 2 * span] + meta[3:4] * gains[0] + meta[5:6] * gains[1]
            rollup[2] = mixed[2 * span : 3 * span] + meta[4:5] * gains[2] + meta[6:7] * gains[3]
            rollup[3] = mixed[3 * span : 4 * span] + meta[1:2] * gains[4] + meta[2:3] * gains[5]
            copy = pltpu.make_async_copy(rollup, rollup_hbm, rollup_sem.at[0])
            copy.start()
            stores.append(copy)
    for copy in stores:
        copy.wait()


def apply(slices, wide, sales, carry, near, meta, mixer, gains):
    span, lanes = sales.shape[1:]
    steps = 8 if slices % 8 == 0 else 1
    anywhere = pl.BlockSpec(memory_space=pl.ANY)
    cube_shape = jax.ShapeDtypeStruct(sales.shape, F32)
    cube = pltpu.VMEM(sales.shape, F32)
    dma = pltpu.SemaphoreType.DMA
    return pl.pallas_call(
        functools.partial(apply_kernel, wide, steps),
        out_shape=(cube_shape,) * 4 + (jax.ShapeDtypeStruct((4, span, lanes), F32),),
        in_specs=[anywhere] * 6,
        out_specs=(anywhere,) * 5,
        scratch_shapes=[
            cube,
            pltpu.VMEM((slices,) + carry.shape[1:], F32),
            pltpu.VMEM(near.shape, F32),
            pltpu.VMEM(meta.shape, F32),
            pltpu.VMEM(mixer.shape, mixer.dtype),
            pltpu.VMEM(gains.shape, F32),
            cube, cube, cube, cube,
            pltpu.VMEM((4, span, lanes), F32),
            dma((steps,)), dma((5,)), dma((steps, 4)), dma((1,)),
        ],
        name="apply",
    )(sales, carry, near, meta, mixer, gains)


def solution(mesh):
    n, n_prod = mesh.shape["date"], mesh.shape["prod"]

    def local(sales, week, month, year):
        slices = min(n, sales.shape[0] // 8)
        wide = n * sales.shape[1] // 300 + 1 > 2
        passed = exchange(n, n_prod, slices, wide, week, month, year, sales)
        return apply(slices, wide, sales, *passed)

    return jax.shard_map(
        local,
        mesh=mesh,
        in_specs=(P("prod", "date", None), P("date"), P("date"), P("date")),
        out_specs=(P("prod", "date", None),) * 4 + (P(None, "date", None),),
        check_vma=False,
    )
```
